16 devices in a mesh: rep: 4 (over y, z, core), dp: 4 (over x).
Axes of the slice: x: 4, y: 2, z: 1, core: 2. Of those that a mesh axis runs over, the one named last changes fastest.
The devices are a block of a 4x4x8 slice.
Arguments:
- x: bfloat16 [16, 2048, 1280], P(('rep', 'dp')), parts along dimension 0
- dy: bfloat16 [16, 2048, 1280], P(('rep', 'dp')), parts along dimension 0
- w_gate: bfloat16 [2, 1280, 3456], P(None, 'dp')
- w_up: bfloat16 [2, 1280, 3456], P(None, 'dp')
- w_down: bfloat16 [2, 3456, 1280], P(None, 'dp')
- m_w_gate: float32 [2, 1280, 3456], P(None, 'dp')
- m_w_up: float32 [2, 1280, 3456], P(None, 'dp')
- m_w_down: float32 [2, 3456, 1280], P(None, 'dp')
- v_w_gate: float32 [2, 1280, 3456], P(None, 'dp')
- v_w_up: float32 [2, 1280, 3456], P(None, 'dp')
- v_w_down: float32 [2, 3456, 1280], P(None, 'dp')
Outputs:
- output 1: bfloat16 [8, 1280, 3456], P('rep', 'dp'), parts along dimension 0
- output 2: bfloat16 [8, 1280, 3456], P('rep', 'dp'), parts along dimension 0
- output 3: bfloat16 [8, 3456, 1280], P('rep', 'dp'), parts along dimension 0
- output 4: float32 [8, 1280, 3456], P('rep', 'dp'), parts along dimension 0
- output 5: float32 [8, 1280, 3456], P('rep', 'dp'), parts along dimension 0
- output 6: float32 [8, 3456, 1280], P('rep', 'dp'), parts along dimension 0
- output 7: float32 [8, 1280, 3456], P('rep', 'dp'), parts along dimension 0
- output 8: float32 [8, 1280, 3456], P('rep', 'dp'), parts along dimension 0
- output 9: float32 [8, 3456, 1280], P('rep', 'dp'), parts along dimension 0
There are 4 independent parts. The reference program is written for one: setup_inputs(seed, part) draws one part's arguments, and reference() takes and returns one part's arrays. A program takes and returns all parts, laid end to end along the dimension named above; an argument that names none is the same for every part.
All inputs are finite; a program needn't handle non-finite values.
Results may differ from the reference program's by a relative error of at most 0.02.
Values are sent between devices in bfloat16 or wider.
A program may use at most 768 MiB of HBM per device.

```python
import jax
import jax.numpy as jnp
from jax import lax

SEQUENCES = 4
TOKENS = 2048
D = 1280
FF = 3456
LAYERS = 2
NAMES = ("w_gate", "w_up", "w_down")
SHAPES = {"w_gate": (LAYERS, D, FF), "w_up": (LAYERS, D, FF), "w_down": (LAYERS, FF, D)}


def bump(key, n, height):
    away = (jnp.arange(n, dtype=jnp.int32) - jax.random.randint(key, (), 0, n, jnp.int32)) % n
    return jnp.where(away < n // 8, height, 1.0)


def together(key, own, strength):
    shared = jax.random.normal(key, own.shape[1:], jnp.float32)
    return (own + strength * shared) * lax.rsqrt(1 + strength * strength)


def setup_inputs(seed: int = 0, part: int = 0) -> dict:
    kx, kdy, ka, kb, kz, kf, kh, kl, *keys = jax.random.split(jax.random.key(seed), 8 + 3 * len(NAMES))
    kx, kdy, ka, kb = (jax.random.fold_in(k, part) for k in (kx, kdy, ka, kb))
    kw, km, kv = (keys[i::3] for i in range(3))
    shape = (SEQUENCES, TOKENS, D)
    much_x, much_dy = jax.random.uniform(kz, (2,), jnp.float32, 0.0, 1.0)
    loud = 2.0 ** jax.random.uniform(jax.random.fold_in(kz, 1), (), jnp.float32, -1.0, 2.0)
    layers = 2.0 ** jax.random.uniform(kl, (LAYERS, 1, 1), jnp.float32, -1.0, 1.0)
    x = together(ka, jax.random.normal(kx, shape, jnp.float32), much_x) * bump(kf, D, 4.0)
    dy = together(kb, jax.random.normal(kdy, shape, jnp.float32), much_dy)
    drawn = {"x": x.astype(jnp.bfloat16), "dy": (loud * dy * (SEQUENCES * TOKENS) ** -0.5).astype(jnp.bfloat16)}
    for key, name in zip(kw, NAMES, strict=True):
        w = jax.random.normal(key, SHAPES[name], jnp.float32) * SHAPES[name][1] ** -0.5
        drawn[name] = (w * {"w_gate": 1.0, "w_up": bump(kh, FF, 4.0), "w_down": layers}[name]).astype(jnp.bfloat16)
    for key, name in zip(km, NAMES, strict=True):
        drawn[f"m_{name}"] = 0.1 * jax.random.normal(key, SHAPES[name], jnp.float32)
    for key, name in zip(kv, NAMES, strict=True):
        drawn[f"v_{name}"] = jax.random.uniform(key, SHAPES[name], jnp.float32, 0.005, 0.015)
    return drawn


def matmul(a, w):
    return jnp.dot(a, w, preferred_element_type=jnp.float32).astype(jnp.bfloat16)


def normed(h):
    wide = h.astype(jnp.float32)
    scale = lax.rsqrt(jnp.mean(wide**2, -1, keepdims=True) + 1e-6)
    return (wide * scale).astype(jnp.bfloat16)


def layer(h, w):
    a = normed(h)
    gate = jnp.dot(a, w["w_gate"], preferred_element_type=jnp.float32)
    up = jnp.dot(a, w["w_up"], preferred_element_type=jnp.float32)
    return h + matmul((jax.nn.silu(gate) * up).astype(jnp.bfloat16), w["w_down"])


def adamw(w, m, v, g):
    m = 0.9 * m + 0.1 * g
    v = 0.95 * v + 0.05 * g * g
    step = m * lax.rsqrt(v + 1e-8) + 0.1 * w
    return (w - 0.02 * step).astype(jnp.bfloat16), m, v


def stack(weights, h):
    return lax.scan(lambda h, w: (layer(h, w), None), h, weights)[0]


def reference(x, dy, w_gate, w_up, w_down, m_w_gate, m_w_up, m_w_down, v_w_gate, v_w_up, v_w_down):
    weights = dict(zip(NAMES, (w_gate, w_up, w_down), strict=True))

    def take(so_far, sequence):
        h, by_y = sequence
        _, back = jax.vjp(lambda w: stack(w, h), weights)
        return jax.tree.map(lambda total, term: total + term.astype(jnp.float32), so_far, back(by_y)[0]), None

    none_yet = {name: jnp.zeros(w.shape, jnp.float32) for name, w in weights.items()}
    by_weights, _ = lax.scan(take, none_yet, (x, dy))
    gradients = [by_weights[name].astype(jnp.bfloat16).astype(jnp.float32) for name in NAMES]
    new = [
        adamw(w.astype(jnp.float32), m, v, g)
        for w, m, v, g in zip((w_gate, w_up, w_down), (m_w_gate, m_w_up, m_w_down), (v_w_gate, v_w_up, v_w_down), gradients, strict=True)
    ]
    return tuple(one[which] for which in range(3) for one in new)
```

```python
import jax
import jax.numpy as jnp
from jax import lax
from jax.experimental import pallas as pl
from jax.experimental.pallas import tpu as pltpu
from jax.sharding import PartitionSpec as P


BF, F32 = jnp.bfloat16, jnp.float32
MESH = pl.DeviceIdType.MESH
ROWS = 256
GU_CUTS, DOWN_CUTS, GRAD_CUTS = 3, 2, 9


def dot(a, b, ca, cb):
    return lax.dot_general(a, b, (((ca,), (cb,)), ((), ())), preferred_element_type=F32)


def normed(h):
    wide = h.astype(F32)
    scale = lax.rsqrt(jnp.mean(wide**2, -1, keepdims=True) + 1e-6)
    return (wide * scale).astype(BF)


def gated(gate, up):
    return (jax.nn.silu(gate) * up).astype(BF)


def adamw(w, m, v, g):
    m = 0.9 * m + 0.1 * g
    v = 0.95 * v + 0.05 * g * g
    step = m * lax.rsqrt(v + 1e-8) + 0.1 * w
    return (w - 0.02 * step).astype(BF), m, v


def forward_kernel(n, x_ref, dy_ref, wg, wu, wd, *refs):
    (g0, u0, d0, g1, u1, d1, gate0, up0, gate1, up1, z0, h1, by_d1,
     zbuf, abuf, xbuf, hbuf, wbuf, dbuf, gst, ust, ost, send, recv, lsem, ssem, osem) = refs
    whole = ((g0, u0, d0), (g1, u1, d1))
    tokens, d = abuf.shape
    ff = zbuf.shape[1]
    fc, dc, gc = ff // GU_CUTS, d // DOWN_CUTS, ff // GRAD_CUTS
    steps = tokens // ROWS
    me = lax.axis_index("dp")
    rep = lax.axis_index("rep")
    core = lax.rem(rep, 2)
    left, right, across = lax.rem(me + n - 1, n), lax.rem(me + 1, n), lax.rem(me + 2, n)
    to_left, to_right, to_other = {"dp": left}, {"dp": right}, {"rep": rep + 1 - 2 * core}

    units = [(layer, kind, j) for layer in range(2) for kind, cuts in (("gu", GU_CUTS), ("d", DOWN_CUTS)) for j in range(cuts)]

    def parts(unit):
        layer, kind, j = units[unit]
        if kind == "gu":
            cols = pl.ds(j * fc, fc)
            return [(whole[layer][0], wg.at[layer], cols), (whole[layer][1], wu.at[layer], cols)]
        return [(whole[layer][2], wd.at[layer], pl.ds(j * dc, dc))]

    def at(start, size):
        return pl.ds(pl.multiple_of(start, 16), size)

    def copies(unit):
        out = []
        for p, (w, block, cols) in enumerate(parts(unit)):
            rows = block.shape[0]
            half = rows // 2
            a = (half // 2 + 15) // 16 * 16
            s = core * half

            def move(k, src, dst, to, p=p):
                return pltpu.make_async_remote_copy(
                    src_ref=src, dst_ref=dst, send_sem=send.at[unit, p, k], recv_sem=recv.at[unit, p, k], device_id=to, device_id_type=MESH
                )

            mine, here = block.at[at(s, half), cols], w.at[at(me * rows + s, half), cols]
            first, second = w.at[at(left * rows + s, a), cols], w.at[at(right * rows + s + a, half - a), cols]
            trade = [w.at[at(b * rows + s, half), cols] for b in (left, right, across)]
            out.append(
                [move(0, mine, here, to_right), move(1, mine, here, to_left), move(2, first, first, to_right), move(3, second, second, to_left)]
                + [move(4 + i, t, t, to_other) for i, t in enumerate(trade)]
            )
        return out

    def A(unit):
        for c in copies(unit):
            c[0].start()
            c[1].start()

    def B(unit):
        for c in copies(unit):
            c[0].wait_recv()
            c[2].start()
            c[1].wait_recv()
            c[3].start()
        for c in copies(unit):
            c[4].start()
            c[5].start()

    def C(unit):
        for c in copies(unit):
            c[2].wait_recv()
            c[3].wait_recv()
            c[6].start()

    def D(unit):
        for c in copies(unit):
            for k in (4, 5, 6):
                c[k].wait_recv()

    stay = []
    for layer in range(2):
        for i, w in enumerate((wg, wu)):
            rows = w.shape[1]
            stay.append((w.at[layer], zbuf.at[pl.ds((2 * layer + i) * rows, rows)], whole[layer][i].at[at(me * rows, rows)]))
        rows = wd.shape[1]
        stay.append((wd.at[layer], hbuf.at[pl.ds(layer * rows, rows)], whole[layer][2].at[at(me * rows, rows)]))

    barrier = pltpu.get_barrier_semaphore()
    for to in (to_left, to_right, to_other):
        pl.semaphore_signal(barrier, inc=1, device_id=to, device_id_type=MESH)
    pl.semaphore_wait(barrier, 3)

    A(0)
    take = pltpu.make_async_copy(x_ref, xbuf, lsem.at[6])
    take.start()
    ins = [pltpu.make_async_copy(src, mid, lsem.at[i]) for i, (src, mid, _) in enumerate(stay)]
    outs = [pltpu.make_async_copy(mid, dst, lsem.at[i]) for i, (_, mid, dst) in enumerate(stay)]
    for c in ins:
        c.start()
    for i, c in enumerate(ins):
        c.wait()
        outs[i].start()
    take.wait()

    def norm(src):
        @pl.loop(0, steps)
        def _(i):
            rows = pl.ds(pl.multiple_of(i * ROWS, ROWS), ROWS)
            abuf[rows, :] = normed(src[rows, :])

    norm(xbuf)
    for c in outs:
        c.wait()
    B(0)
    A(1)

    def ready(unit):
        C(unit)
        D(unit)

    def hook(unit):
        B(unit + 1)
        if unit + 2 < len(units):
            A(unit + 2)

    def gate_up(layer, gate, up, base):
        wgate, wup, _ = whole[layer]

        @pl.loop(0, GU_CUTS)
        def _(j):
            for jj in range(GU_CUTS):
                pl.when(j == jj)(lambda u=base + jj: ready(u))
            cols = pl.ds(pl.multiple_of(j * fc, 128), fc)
            ga = pltpu.make_async_copy(wgate.at[:, cols], wbuf.at[0], lsem.at[0])
            ua = pltpu.make_async_copy(wup.at[:, cols], wbuf.at[1], lsem.at[1])
            ga.start()
            ua.start()
            ga.wait()
            ua.wait()

            @pl.loop(0, steps)
            def _(i):
                for jj in range(GU_CUTS):
                    pl.when((j == jj) & (i == steps - 2))(lambda u=base + jj: hook(u))
                rows = pl.ds(pl.multiple_of(i * ROWS, ROWS), ROWS)
                slot = lax.rem(i, 2)
                put_g = pltpu.make_async_copy(gst.at[slot], gate.at[rows, cols], ssem.at[0, slot])
                put_u = pltpu.make_async_copy(ust.at[slot], up.at[rows, cols], ssem.at[1, slot])

                @pl.when(i >= 2)
                def _():
                    put_g.wait()
                    put_u.wait()

                g = dot(abuf[rows, :], wbuf[0], 1, 0)
                u = dot(abuf[rows, :], wbuf[1], 1, 0)
                gst[slot] = g
                ust[slot] = u
                zbuf[rows, cols] = gated(g, u)
                put_g.start()
                put_u.start()

            for slot in range(2):
                rows = pl.ds(slot * ROWS, ROWS)
                pltpu.make_async_copy(gst.at[slot], gate.at[rows, cols], ssem.at[0, slot]).wait()
                pltpu.make_async_copy(ust.at[slot], up.at[rows, cols], ssem.at[1, slot]).wait()

    gate_up(0, gate0, up0, 0)
    put_z = pltpu.make_async_copy(zbuf, z0, lsem.at[2])
    put_z.start()

    @pl.loop(0, DOWN_CUTS)
    def _(j):
        for jj in range(DOWN_CUTS):
            pl.when(j == jj)(lambda u=GU_CUTS + jj: ready(u))
        cols = pl.ds(pl.multiple_of(j * dc, 128), dc)
        da = pltpu.make_async_copy(d0.at[:, cols], dbuf, lsem.at[0])
        da.start()
        da.wait()

        @pl.loop(0, steps)
        def _(i):
            for jj in range(DOWN_CUTS):
                pl.when((j == jj) & (i == steps - 2))(lambda u=GU_CUTS + jj: hook(u))
            rows = pl.ds(pl.multiple_of(i * ROWS, ROWS), ROWS)
            hbuf[rows, cols] = xbuf[rows, cols] + dot(zbuf[rows, :], dbuf[...], 1, 0).astype(BF)

    put_h = pltpu.make_async_copy(hbuf, h1, lsem.at[3])
    put_h.start()
    take = pltpu.make_async_copy(dy_ref, xbuf, lsem.at[6])
    take.start()
    norm(hbuf)
    put_z.wait()
    gate_up(1, gate1, up1, GU_CUTS + DOWN_CUTS)
    take.wait()
    last = len(units) - 1

    @pl.loop(0, GRAD_CUTS)
    def _(t):
        pl.when(t == 2)(lambda: B(last))
        pl.when(t == 5)(lambda: C(last - 1))
        cols = pl.ds(pl.multiple_of(t * gc, 128), gc)
        slot = lax.rem(t, 2)
        put = pltpu.make_async_copy(ost.at[slot], by_d1.at[pl.ds(pl.multiple_of(t * gc, 128), gc)], osem.at[slot])
        pl.when(t >= 2)(lambda: put.wait())
        ost[slot] = dot(zbuf[:, cols], xbuf[...], 0, 0).astype(BF)
        put.start()

    for slot in range(2):
        pltpu.make_async_copy(ost.at[slot], by_d1.at[pl.ds(slot * gc, gc)], osem.at[slot]).wait()
    D(last - 1)
    C(last)
    D(last)
    put_h.wait()
    for unit in range(len(units)):
        for c in copies(unit):
            for one in c:
                one.wait_send()


def forward(n, x, dy, wg, wu, wd):
    tokens, d = x.shape
    layers, _, ff = wg.shape
    fc, dc, gc = ff // GU_CUTS, d // DOWN_CUTS, ff // GRAD_CUTS
    n_units = layers * (GU_CUTS + DOWN_CUTS)
    out = lambda *shape, dtype=BF: jax.ShapeDtypeStruct(shape, dtype)
    layer = [out(d, ff), out(d, ff), out(ff, d)]
    pre = [out(tokens, ff, dtype=F32)] * 4
    flops = 2 * tokens * d * ff * 6
    return pl.pallas_call(
        lambda *refs: forward_kernel(n, *refs),
        out_shape=layer + layer + pre + [out(tokens, ff), out(tokens, d), out(ff, d)],
        in_specs=[pl.BlockSpec(memory_space=pl.ANY)] * 5,
        out_specs=[pl.BlockSpec(memory_space=pl.ANY)] * 13,
        scratch_shapes=[
            pltpu.VMEM((tokens, ff), BF),
            pltpu.VMEM((tokens, d), BF),
            pltpu.VMEM((tokens, d), BF),
            pltpu.VMEM((tokens, d), BF),
            pltpu.VMEM((2, d, fc), BF),
            pltpu.VMEM((ff, dc), BF),
            pltpu.VMEM((2, ROWS, fc), F32),
            pltpu.VMEM((2, ROWS, fc), F32),
            pltpu.VMEM((2, gc, d), BF),
            pltpu.SemaphoreType.DMA((n_units, 2, 7)),
            pltpu.SemaphoreType.DMA((n_units, 2, 7)),
            pltpu.SemaphoreType.DMA((7,)),
            pltpu.SemaphoreType.DMA((2, 2)),
            pltpu.SemaphoreType.DMA((2,)),
        ],
        compiler_params=pltpu.CompilerParams(collective_id=0, has_side_effects=True, vmem_limit_bytes=67043328),
        cost_estimate=pl.CostEstimate(flops=flops, bytes_accessed=300_000_000, transcendentals=0),
        name="gather_forward",
    )(x, dy, wg, wu, wd)


def solution(mesh):
    n = mesh.shape["dp"]

    def scattered(g):
        return lax.psum_scatter(g, "dp", scatter_dimension=0, tiled=True)

    def step(x, dy, *arrays):
        weights, m, v = (arrays[i : i + 3] for i in (0, 3, 6))
        x, dy = x[0], dy[0]
        _, _, d0, g1, u1, d1, gate0, up0, gate1, up1, z0, h1, by_d1 = forward(n, x, dy, *weights)
        sum_d1 = scattered(by_d1)
        a0 = normed(x)
        a1, back_a1 = jax.vjp(normed, h1)

        by_z1 = dot(dy, d1, 1, 1).astype(BF)
        by_gate1, by_up1 = (t.astype(BF) for t in jax.vjp(gated, gate1, up1)[1](by_z1))
        by_g1 = dot(a1, by_gate1, 0, 0).astype(BF)
        sum_g1 = scattered(by_g1)
        by_u1 = dot(a1, by_up1, 0, 0).astype(BF)
        by_u1, by_g1, by_gate1, by_up1 = lax.optimization_barrier((by_u1, by_g1, by_gate1, by_up1))
        sum_u1 = scattered(by_u1)
        by_a1 = dot(by_gate1, g1, 1, 1).astype(BF) + dot(by_up1, u1, 1, 1).astype(BF)
        by_h1 = dy + back_a1(by_a1)[0]
        by_d0 = dot(z0, by_h1, 0, 0).astype(BF)
        sum_d0 = scattered(by_d0)
        by_z0 = dot(by_h1, d0, 1, 1).astype(BF)
        by_gate0, by_up0 = (t.astype(BF) for t in jax.vjp(gated, gate0, up0)[1](by_z0))
        sum_g0 = scattered(dot(a0, by_gate0, 0, 0).astype(BF))
        sum_u0 = scattered(dot(a0, by_up0, 0, 0).astype(BF))

        gradients = [jnp.stack(pair).astype(F32) for pair in ((sum_g0, sum_g1), (sum_u0, sum_u1), (sum_d0, sum_d1))]
        new = [adamw(w.astype(F32), m, v, g) for w, m, v, g in zip(weights, m, v, gradients, strict=True)]
        return tuple(one[which] for which in range(3) for one in new)

    states, cut = P(("rep", "dp"), None, None), P(None, "dp", None)
    return jax.shard_map(
        step,
        mesh=mesh,
        in_specs=(states, states) + (cut,) * 9,
        out_specs=(P("rep", "dp", None),) * 9,
        check_vma=False,
    )
```

```python
import jax
import jax.numpy as jnp
from jax import lax
from jax.experimental import pallas as pl
from jax.experimental.pallas import tpu as pltpu
from jax.sharding import PartitionSpec as P


BF, F32 = jnp.bfloat16, jnp.float32
MESH = pl.DeviceIdType.MESH
ROWS = 256
GU_CUTS, DOWN_CUTS, GRAD_CUTS = 3, 2, 9


def dot(a, b, ca, cb):
    return lax.dot_general(a, b, (((ca,), (cb,)), ((), ())), preferred_element_type=F32)


def normed(h):
    wide = h.astype(F32)
    scale = lax.rsqrt(jnp.mean(wide**2, -1, keepdims=True) + 1e-6)
    return (wide * scale).astype(BF)


def gated(gate, up):
    return (jax.nn.silu(gate) * up).astype(BF)


def adamw(w, m, v, g):
    m = 0.9 * m + 0.1 * g
    v = 0.95 * v + 0.05 * g * g
    step = m * lax.rsqrt(v + 1e-8) + 0.1 * w
    return (w - 0.02 * step).astype(BF), m, v


def forward_kernel(n, x_ref, dy_ref, wg, wu, wd, *refs):
    (g0, u0, d0, g1, u1, d1, gate0, up0, gate1, up1, z0, h1, by_d1,
     zbuf, abuf, xbuf, hbuf, wbuf, dbuf, gst, ust, ost, send, recv, lsem, ssem, osem) = refs
    whole = ((g0, u0, d0), (g1, u1, d1))
    tokens, d = abuf.shape
    ff = zbuf.shape[1]
    fc, dc, gc = ff // GU_CUTS, d // DOWN_CUTS, ff // GRAD_CUTS
    steps = tokens // ROWS
    me = lax.axis_index("dp")
    rep = lax.axis_index("rep")
    core = lax.rem(rep, 2)
    chip = lax.rem(rep // 2, 2)
    left, right, across = lax.rem(me + n - 1, n), lax.rem(me + 1, n), lax.rem(me + 2, n)
    to_left, to_right, to_other = {"dp": left}, {"dp": right}, {"rep": rep + 1 - 2 * core}
    to_chip = {"rep": rep + 2 - 4 * chip}

    units = [(layer, kind, j) for layer in range(2) for kind, cuts in (("gu", GU_CUTS), ("d", DOWN_CUTS)) for j in range(cuts)]

    def parts(unit):
        layer, kind, j = units[unit]
        if kind == "gu":
            cols = pl.ds(j * fc, fc)
            return [(whole[layer][0], wg.at[layer], cols), (whole[layer][1], wu.at[layer], cols)]
        return [(whole[layer][2], wd.at[layer], pl.ds(j * dc, dc))]

    def at(start, size):
        return pl.ds(pl.multiple_of(start, 16), size)

    part_at = [0]
    for unit in range(len(units)):
        part_at.append(part_at[-1] + len(parts(unit)))

    def copies(unit, kinds):
        out = []
        for p, (w, block, cols) in enumerate(parts(unit)):
            rows = block.shape[0]
            half = rows // 2
            strip = half // 3 // 16 * 16
            size = half - strip
            a = (size // 2 + 15) // 16 * 16
            s = core * half + chip * strip
            given, got = core * half + chip * size, core * half + (1 - chip) * size
            index = part_at[unit] + p

            def move(k):
                if k < 2:
                    src, dst = block.at[at(s, size), cols], w.at[at(me * rows + s, size), cols]
                    to = (to_right, to_left)[k]
                elif k < 4:
                    src = dst = w.at[at(left * rows + s, a), cols] if k == 2 else w.at[at(right * rows + s + a, size - a), cols]
                    to = (to_right, to_left)[k - 2]
                else:
                    b = (left, right, across)[(k - 4) % 3]
                    start, count, to = ((s, size, to_other), (given, strip, to_chip), (got, strip, to_other))[(k - 4) // 3]
                    src = dst = w.at[at(b * rows + start, count), cols]
                return pltpu.make_async_remote_copy(
                    src_ref=src, dst_ref=dst, send_sem=send.at[index, k], recv_sem=recv.at[index, k], device_id=to, device_id_type=MESH
                )

            out.append([move(k) for k in kinds])
        return out

    def start(unit, *kinds):
        for c in copies(unit, kinds):
            for one in c:
                one.start()

    def arrived(unit, *kinds):
        for c in copies(unit, kinds):
            for one in c:
                one.wait_recv()

    def A(unit):
        start(unit, 0, 1)

    def B(unit):
        arrived(unit, 0, 1)
        start(unit, 2, 3)
        start(unit, 7, 8)
        start(unit, 4, 5)

    def C(unit):
        arrived(unit, 2, 3)
        start(unit, 9, 6)

    def E(unit):
        arrived(unit, 7, 8, 9)
        start(unit, 10, 11, 12)

    def D(unit):
        arrived(unit, 4, 5, 6, 10, 11, 12)

    stay = []
    for layer in range(2):
        for i, w in enumerate((wg, wu)):
            rows = w.shape[1]
            stay.append((w.at[layer], zbuf.at[pl.ds((2 * layer + i) * rows, rows)], whole[layer][i].at[at(me * rows, rows)]))
        rows = wd.shape[1]
        stay.append((wd.at[layer], hbuf.at[pl.ds(layer * rows, rows)], whole[layer][2].at[at(me * rows, rows)]))

    barrier = pltpu.get_barrier_semaphore()
    for to in (to_left, to_right, to_other, to_chip):
        pl.semaphore_signal(barrier, inc=1, device_id=to, device_id_type=MESH)
    pl.semaphore_wait(barrier, 4)

    A(0)
    take = pltpu.make_async_copy(x_ref, xbuf, lsem.at[6])
    take.start()
    ins = [pltpu.make_async_copy(src, mid, lsem.at[i]) for i, (src, mid, _) in enumerate(stay)]
    outs = [pltpu.make_async_copy(mid, dst, lsem.at[i]) for i, (_, mid, dst) in enumerate(stay)]
    for c in ins:
        c.start()
    for i, c in enumerate(ins):
        c.wait()
        outs[i].start()
    take.wait()

    def norm(src):
        @pl.loop(0, steps)
        def _(i):
            rows = pl.ds(pl.multiple_of(i * ROWS, ROWS), ROWS)
            abuf[rows, :] = normed(src[rows, :])

    norm(xbuf)
    for c in outs:
        c.wait()
    B(0)
    A(1)

    C(0)
    E(0)
    B(1)
    A(2)
    hooks = {
        steps - 5: lambda unit: C(unit + 1),
        steps - 2: lambda unit: E(unit + 1),
        steps - 1: lambda unit: (B(unit + 2), A(unit + 3) if unit + 3 < len(units) else None),
    }

    def pump(j, cuts, i, base):
        for jj in range(cuts):
            for step, hook in hooks.items():
                pl.when((j == jj) & (i == step))(lambda u=base + jj, hook=hook: (hook(u), None)[1])

    def gate_up(layer, gate, up, base):
        wgate, wup, _ = whole[layer]

        @pl.loop(0, GU_CUTS)
        def _(j):
            for jj in range(GU_CUTS):
                pl.when(j == jj)(lambda u=base + jj: D(u))
            cols = pl.ds(pl.multiple_of(j * fc, 128), fc)
            ga = pltpu.make_async_copy(wgate.at[:, cols], wbuf.at[0], lsem.at[0])
            ua = pltpu.make_async_copy(wup.at[:, cols], wbuf.at[1], lsem.at[1])
            ga.start()
            ua.start()
            ga.wait()
            ua.wait()

            @pl.loop(0, steps)
            def _(i):
                pump(j, GU_CUTS, i, base)
                rows = pl.ds(pl.multiple_of(i * ROWS, ROWS), ROWS)
                slot = lax.rem(i, 2)
                put_g = pltpu.make_async_copy(gst.at[slot], gate.at[rows, cols], ssem.at[0, slot])
                put_u = pltpu.make_async_copy(ust.at[slot], up.at[rows, cols], ssem.at[1, slot])

                @pl.when(i >= 2)
                def _():
                    put_g.wait()
                    put_u.wait()

                g = dot(abuf[rows, :], wbuf[0], 1, 0)
                u = dot(abuf[rows, :], wbuf[1], 1, 0)
                gst[slot] = g
                ust[slot] = u
                zbuf[rows, cols] = gated(g, u)
                put_g.start()
                put_u.start()

            for slot in range(2):
                rows = pl.ds(slot * ROWS, ROWS)
                pltpu.make_async_copy(gst.at[slot], gate.at[rows, cols], ssem.at[0, slot]).wait()
                pltpu.make_async_copy(ust.at[slot], up.at[rows, cols], ssem.at[1, slot]).wait()

    gate_up(0, gate0, up0, 0)
    put_z = pltpu.make_async_copy(zbuf, z0, lsem.at[2])
    put_z.start()

    @pl.loop(0, DOWN_CUTS)
    def _(j):
        for jj in range(DOWN_CUTS):
            pl.when(j == jj)(lambda u=GU_CUTS + jj: D(u))
        cols = pl.ds(pl.multiple_of(j * dc, 128), dc)
        da = pltpu.make_async_copy(d0.at[:, cols], dbuf, lsem.at[0])
        da.start()
        da.wait()

        @pl.loop(0, steps)
        def _(i):
            pump(j, DOWN_CUTS, i, GU_CUTS)
            rows = pl.ds(pl.multiple_of(i * ROWS, ROWS), ROWS)
            hbuf[rows, cols] = xbuf[rows, cols] + dot(zbuf[rows, :], dbuf[...], 1, 0).astype(BF)

    put_h = pltpu.make_async_copy(hbuf, h1, lsem.at[3])
    put_h.start()
    take = pltpu.make_async_copy(dy_ref, xbuf, lsem.at[6])
    take.start()
    norm(hbuf)
    put_z.wait()
    gate_up(1, gate1, up1, GU_CUTS + DOWN_CUTS)
    take.wait()
    last = len(units) - 1

    @pl.loop(0, GRAD_CUTS)
    def _(t):
        pl.when(t == 2)(lambda: C(last))
        pl.when(t == 4)(lambda: E(last))
        cols = pl.ds(pl.multiple_of(t * gc, 128), gc)
        slot = lax.rem(t, 2)
        put = pltpu.make_async_copy(ost.at[slot], by_d1.at[pl.ds(pl.multiple_of(t * gc, 128), gc)], osem.at[slot])
        pl.when(t >= 2)(lambda: put.wait())
        ost[slot] = dot(zbuf[:, cols], xbuf[...], 0, 0).astype(BF)
        put.start()

    for slot in range(2):
        pltpu.make_async_copy(ost.at[slot], by_d1.at[pl.ds(slot * gc, gc)], osem.at[slot]).wait()
    D(last - 1)
    D(last)
    put_h.wait()
    for unit in range(len(units)):
        for c in copies(unit, range(13)):
            for one in c:
                one.wait_send()


def forward(n, x, dy, wg, wu, wd):
    tokens, d = x.shape
    layers, _, ff = wg.shape
    fc, dc, gc = ff // GU_CUTS, d // DOWN_CUTS, ff // GRAD_CUTS
    n_parts = layers * (2 * GU_CUTS + DOWN_CUTS)
    out = lambda *shape, dtype=BF: jax.ShapeDtypeStruct(shape, dtype)
    layer = [out(d, ff), out(d, ff), out(ff, d)]
    pre = [out(tokens, ff, dtype=F32)] * 4
    flops = 2 * tokens * d * ff * 6
    return pl.pallas_call(
        lambda *refs: forward_kernel(n, *refs),
        out_shape=layer + layer + pre + [out(tokens, ff), out(tokens, d), out(ff, d)],
        in_specs=[pl.BlockSpec(memory_space=pl.ANY)] * 5,
        out_specs=[pl.BlockSpec(memory_space=pl.ANY)] * 13,
        scratch_shapes=[
            pltpu.VMEM((tokens, ff), BF),
            pltpu.VMEM((tokens, d), BF),
            pltpu.VMEM((tokens, d), BF),
            pltpu.VMEM((tokens, d), BF),
            pltpu.VMEM((2, d, fc), BF),
            pltpu.VMEM((ff, dc), BF),
            pltpu.VMEM((2, ROWS, fc), F32),
            pltpu.VMEM((2, ROWS, fc), F32),
            pltpu.VMEM((2, gc, d), BF),
            pltpu.SemaphoreType.DMA((n_parts, 13)),
            pltpu.SemaphoreType.DMA((n_parts, 13)),
            pltpu.SemaphoreType.DMA((7,)),
            pltpu.SemaphoreType.DMA((2, 2)),
            pltpu.SemaphoreType.DMA((2,)),
        ],
        compiler_params=pltpu.CompilerParams(collective_id=0, has_side_effects=True, vmem_limit_bytes=67043328),
        cost_estimate=pl.CostEstimate(flops=flops, bytes_accessed=300_000_000, transcendentals=0),
        name="gather_forward",
    )(x, dy, wg, wu, wd)


def updated(layer, w, m, v, g, before=()):
    _, rows, columns = w.shape
    size = 64 if rows % 64 == 0 else 96

    def kernel(w_ref, m_ref, v_ref, g_ref, *refs):
        for ref, new in zip(refs[-3:], adamw(w_ref[...].astype(F32), m_ref[...], v_ref[...], g_ref[...].astype(F32)), strict=True):
            ref[...] = new

    place = pl.BlockSpec((None, size, columns), lambda i: (layer, i, 0))
    return pl.pallas_call(
        kernel,
        grid=(rows // size,),
        out_shape=[jax.ShapeDtypeStruct(t.shape, t.dtype) for t in (w, m, v)],
        in_specs=[place, place, place, pl.BlockSpec((size, columns), lambda i: (i, 0))] + [pl.BlockSpec(memory_space=pl.ANY)] * len(before),
        out_specs=[place] * 3,
        input_output_aliases={4 + i: i for i in range(len(before))},
        compiler_params=pltpu.CompilerParams(dimension_semantics=("arbitrary",)),
        cost_estimate=pl.CostEstimate(flops=8_000_000_000, bytes_accessed=22 * rows * columns, transcendentals=rows * columns),
        name="adamw",
    )(w, m, v, g, *before)


def solution(mesh):
    n = mesh.shape["dp"]

    def scattered(g):
        return lax.psum_scatter(g, "dp", scatter_dimension=0, tiled=True)

    def step(x, dy, *arrays):
        weights, m, v = (arrays[i : i + 3] for i in (0, 3, 6))
        x, dy = x[0], dy[0]
        _, _, d0, g1, u1, d1, gate0, up0, gate1, up1, z0, h1, by_d1 = forward(n, x, dy, *weights)
        sum_d1 = scattered(by_d1)
        a0 = normed(x)
        a1, back_a1 = jax.vjp(normed, h1)

        by_z1 = dot(dy, d1, 1, 1).astype(BF)
        by_gate1, by_up1 = (t.astype(BF) for t in jax.vjp(gated, gate1, up1)[1](by_z1))
        by_g1 = dot(a1, by_gate1, 0, 0).astype(BF)
        sum_g1 = scattered(by_g1)
        by_u1 = dot(a1, by_up1, 0, 0).astype(BF)
        by_u1, by_g1, by_gate1, by_up1 = lax.optimization_barrier((by_u1, by_g1, by_gate1, by_up1))
        sum_u1 = scattered(by_u1)
        by_a1 = dot(by_gate1, g1, 1, 1).astype(BF) + dot(by_up1, u1, 1, 1).astype(BF)
        by_h1 = dy + back_a1(by_a1)[0]
        by_d0 = dot(z0, by_h1, 0, 0).astype(BF)
        sum_d0 = scattered(by_d0)
        by_z0 = dot(by_h1, d0, 1, 1).astype(BF)
        by_gate0, by_up0 = (t.astype(BF) for t in jax.vjp(gated, gate0, up0)[1](by_z0))
        sum_g0 = scattered(dot(a0, by_gate0, 0, 0).astype(BF))
        sum_u0 = scattered(dot(a0, by_up0, 0, 0).astype(BF))

        new = []
        for w, m, v, layers in zip(weights, m, v, ((sum_g0, sum_g1), (sum_u0, sum_u1), (sum_d0, sum_d1)), strict=True):
            new.append(updated(0, w, m, v, layers[0], updated(1, w, m, v, layers[1])))
        return tuple(one[which] for which in range(3) for one in new)

    states, cut = P(("rep", "dp"), None, None), P(None, "dp", None)
    return jax.shard_map(
        step,
        mesh=mesh,
        in_specs=(states, states) + (cut,) * 9,
        out_specs=(P("rep", "dp", None),) * 9,
        check_vma=False,
    )
```
